32 devices in a mesh: dp: 8 (over z, y), mp: 4 (over x, core).
Axes of the slice: x: 2, y: 2, z: 4, core: 2. Of those that a mesh axis runs over, the one named last changes fastest.
Arguments:
- hidden_input: bfloat16 [8192, 24], P('dp'), may hold values from -6 to 6
- output_cotangent: bfloat16 [8192, 8192], P('dp', 'mp'), may hold values from -0.023925781 to 0.023925781
- master_weights: float32 [24, 8192], P('dp', 'mp'), may hold values from -6 to 6
- first_codes: int32 [24, 8192], P('dp', 'mp'), may hold values from 0 to 15
- second_codes: int32 [24, 8192], P('dp', 'mp'), may hold values from 0 to 15
- first_rows: float32 [24], P('dp'), may hold values from 0.001 to 0.03
- first_cols: float32 [8192], P('mp'), may hold values from 0.001 to 0.03
- second_rows: float32 [24], P('dp'), may hold values from 1e-05 to 0.001
- second_cols: float32 [8192], P('mp'), may hold values from 1e-05 to 0.001
- step_count: int32 [], replicated, may hold values from 1 to 9
Outputs:
- new_master: float32 [24, 8192], P('dp', 'mp')
- update_ratio: float32 [24, 8192], P('dp', 'mp')
- gathered_params: bfloat16 [24, 8192], P(None, 'mp')
- first_scaled: float32 [24, 8192], P('dp', 'mp')
- second_scaled: float32 [24, 8192], P('dp', 'mp')
- new_first_rows: float32 [24], P('dp')
- new_first_cols: float32 [8192], P('mp')
- new_second_rows: float32 [24], P('dp')
- new_second_cols: float32 [8192], P('mp')
The draws below stay inside these ranges and needn't reach their ends.
All inputs are finite; a program needn't handle non-finite values.
Results may differ from the reference program's by a relative error of at most 0.001.
Values may be sent and summed in bfloat16 or wider, within the bound.
A program may use at most 64 MiB of HBM per device.

```python
import math
import jax
import jax.numpy as jnp
from jax import lax

D = 8192
ROWS = 24
TOKENS = 8192


def plant(values, own_key, low, high):
    longest = values.shape.index(max(values.shape))
    spots = []
    for shift in (0, 1):
        where = [jax.random.randint(jax.random.fold_in(own_key, axis), (), 0, length) for axis, length in enumerate(values.shape)]
        where[longest] = (where[longest] + shift) % values.shape[longest]
        spots.append(tuple(where))
    return values.at[spots[0]].set(low).at[spots[1]].set(high)


def spiked(values, own_key, source, target, parts, factor):
    def block_of(axis_at):
        return (jnp.arange(values.shape[axis_at]) // (values.shape[axis_at] // parts)).reshape((-1,) + (1,) * (values.ndim - 1 - axis_at))

    one_side = jax.random.permutation(own_key, parts)[block_of(target)]
    far = (block_of(target) + parts // 2) % parts
    return jnp.where((block_of(source) == one_side) | (block_of(source) == far), factor * values, values)


def block_scale(key, extent, pieces, smallest, high):
    loudness, own = 1.0, jax.random.fold_in(key, 6)
    for axis_at, parts in pieces:
        draws = jnp.exp(jax.random.uniform(jax.random.fold_in(own, axis_at), (parts,), jnp.float32, smallest / len(pieces), high / len(pieces)))
        loudness = loudness * jnp.repeat(draws, extent[axis_at] // parts).reshape([-1 if axis == axis_at else 1 for axis in range(len(extent))])
    return loudness


def bell_draw(stream_key, dims, deviation, most, split=(), kind=jnp.bfloat16):
    values = jax.random.normal(stream_key, dims, jnp.float32) * deviation
    if len(split) > 0:
        values = block_scale(stream_key, dims, split, -0.22, 0.18) * values
    return jnp.clip(values, min=-most, max=most).astype(kind)


def noise_with(own_key, extent, deviation, reach, shards, heavy, dtype=jnp.bfloat16):
    result = deviation * jax.random.normal(own_key, extent, jnp.float32)
    if shards:
        result = result * block_scale(own_key, extent, shards, -0.22, 0.18)
    return jnp.clip(spiked(result, jax.random.fold_in(own_key, 3), *heavy), -reach, reach).astype(dtype)


def setup_inputs(seed: int = 0) -> dict:
    splits = jax.random.split(jax.random.key(seed), 11)
    return {
        "hidden_input": noise_with(splits[0], (TOKENS, ROWS), 1.0, 6.0, ((0, 8),), (0, 1, 8, 2.0)),
        "output_cotangent": bell_draw(splits[1], (TOKENS, D), 0.004, 0.023925781, ((0, 8), (1, 4))),
        "master_weights": bell_draw(splits[2], (ROWS, D), 1.0, 6.0, ((0, 8), (1, 4)), jnp.float32),
        "first_codes": plant(jax.random.randint(splits[3], (ROWS, D), 0, 16), jax.random.fold_in(splits[3], 1), 0, 15).astype(jnp.int32),
        "second_codes": plant(jax.random.randint(splits[4], (ROWS, D), 0, 16), jax.random.fold_in(splits[4], 1), 0, 15).astype(jnp.int32),
        "first_rows": jnp.clip(jnp.exp(math.log(0.03) - 3.4011973 * jax.random.uniform(splits[5], (ROWS,), jnp.float32) ** block_scale(splits[5], (ROWS,), ((0, 8),), -0.2, 0.2)), 0.001, 0.03),
        "first_cols": jnp.clip(jnp.exp(math.log(0.03) - 3.4011973 * jax.random.uniform(splits[6], (D,), jnp.float32) ** block_scale(splits[6], (D,), ((0, 4),), -0.2, 0.2)), 0.001, 0.03),
        "second_rows": jnp.clip(jnp.exp(math.log(0.001) - 4.6051703 * jax.random.uniform(splits[7], (ROWS,), jnp.float32) ** block_scale(splits[7], (ROWS,), ((0, 8),), -0.2, 0.2)), 9.999999747378752e-06, 0.001),
        "second_cols": jnp.clip(jnp.exp(math.log(0.001) - 4.6051703 * jax.random.uniform(splits[8], (D,), jnp.float32) ** block_scale(splits[8], (D,), ((0, 4),), -0.2, 0.2)), 9.999999747378752e-06, 0.001),
        "step_count": jax.random.randint(splits[9], (), 1, 10).astype(jnp.int32),
    }


def reference(hidden_input, output_cotangent, master_weights, first_codes, second_codes, first_rows, first_cols, second_rows, second_cols, step_count):
    gradient = jnp.dot(hidden_input.T, output_cotangent, preferred_element_type=jnp.float32)
    entries = gradient.shape[0] * gradient.shape[1]
    gnorm = jnp.sqrt(jnp.sum(gradient * gradient))
    clipf = jnp.minimum(1.0, 0.01 * jnp.sqrt(jnp.float32(entries)) / (gnorm + 1e-06))
    clipped = clipf * gradient
    first_old = (first_codes.astype(jnp.float32) - 7.5) / 7.5 * jnp.minimum(first_rows[:, None], first_cols[None, :])
    second_level = (second_codes.astype(jnp.float32) + 1.0) / 16.0
    second_old = second_level * second_level * jnp.minimum(second_rows[:, None], second_cols[None, :])
    first_new = 0.9 * first_old + 0.1 * clipped
    second_new = 0.95 * second_old + 0.05 * clipped * clipped
    steps = step_count.astype(jnp.float32)
    first_fix = 1.0 - jnp.power(jnp.float32(0.9), steps)
    second_fix = 1.0 - jnp.power(jnp.float32(0.95), steps)
    update_ratio = first_new / first_fix / (jnp.sqrt(second_new / second_fix) + 1e-08)
    new_master = master_weights - 0.001 * (update_ratio + 0.1 * master_weights)
    first_abs = jnp.abs(first_new)
    new_first_rows = lax.optimization_barrier(jnp.max(first_abs, axis=1))
    new_first_cols = lax.optimization_barrier(jnp.max(first_abs, axis=0))
    new_second_rows = lax.optimization_barrier(jnp.max(second_new, axis=1))
    new_second_cols = lax.optimization_barrier(jnp.max(second_new, axis=0))
    first_scaled = first_new / (jnp.minimum(new_first_rows[:, None], new_first_cols[None, :]) + 1e-08)
    second_scaled = second_new / (jnp.minimum(new_second_rows[:, None], new_second_cols[None, :]) + 1e-08)
    gathered_params = new_master.astype(jnp.bfloat16)
    return (new_master, update_ratio, gathered_params, first_scaled, second_scaled, new_first_rows, new_first_cols, new_second_rows, new_second_cols)
```

```python
import functools

import jax
import jax.numpy as jnp
from jax import lax
from jax.experimental import pallas as pl
from jax.experimental.pallas import tpu as pltpu
from jax.sharding import PartitionSpec as P

MESH = pl.DeviceIdType.MESH
F32 = jnp.float32


def kernel(
    ndp,
    nmp,
    chunks,
    hidden_hbm,
    cot_hbm,
    master_hbm,
    code1_hbm,
    code2_hbm,
    cols1_hbm,
    cols2_hbm,
    rows1_ref,
    rows2_ref,
    step_ref,
    master_out,
    ratio_out,
    params_out,
    scaled1_out,
    scaled2_out,
    rows_out,
    newcols1_out,
    newcols2_out,
    hidden,
    cot,
    master,
    code1,
    code2,
    cols1,
    cols2,
    share,
    grads,
    square,
    squares,
    params,
    maxcol,
    maxcols,
    maxrow,
    maxrows,
    old1,
    old2,
    in_sem,
    cot_sem,
    send_sem,
    recv_sem,
):
    dp = lax.axis_index("dp")
    mp = lax.axis_index("mp")
    ndev = ndp * nmp
    flat = dp * nmp + mp
    rows, ncols = master.shape
    width = ncols // chunks

    def loop(count, body):
        def step(i, carry):
            body(i)
            return carry

        lax.fori_loop(0, count, step, 0, unroll=count <= 32)

    loads = []
    for i, (src, dst) in enumerate(
        (
            (hidden_hbm, hidden),
            (code1_hbm, code1),
            (code2_hbm, code2),
            (cols1_hbm, cols1),
            (cols2_hbm, cols2),
            (master_hbm, master),
        )
    ):
        copy = pltpu.make_async_copy(src, dst, in_sem.at[i])
        loads.append(copy)
    cot_loads = [
        pltpu.make_async_copy(
            cot_hbm.at[:, pl.ds(c * width, width)], cot.at[c], cot_sem.at[c]
        )
        for c in range(chunks)
    ]
    loads[0].start()
    for copy in cot_loads:
        copy.start()
    for copy in loads[1:]:
        copy.start()

    def peer(k):
        other = lax.rem(flat + k + 1, ndev)
        return {"dp": lax.div(other, nmp), "mp": lax.rem(other, nmp)}

    barrier = pltpu.get_barrier_semaphore()
    loop(
        ndev - 1,
        lambda k: pl.semaphore_signal(
            barrier, inc=1, device_id=peer(k), device_id_type=MESH
        ),
    )

    def send_share(c):
        cols = pl.ds(c * width, width)

        def body(k):
            to = lax.rem(dp + k + 1, ndp)
            pltpu.make_async_remote_copy(
                src_ref=share.at[to, :, cols],
                dst_ref=grads.at[k, :, cols],
                send_sem=send_sem.at[0],
                recv_sem=recv_sem.at[0],
                device_id={"dp": to},
                device_id_type=MESH,
            ).start()

        return body

    loads[0].wait()
    for c in range(chunks):
        cot_loads[c].wait()
        part = lax.dot_general(
            hidden[...], cot[c], (((1,), (0,)), ((), ())), preferred_element_type=F32
        )
        for j in range(ndp):
            share[j, :, c * width : (c + 1) * width] = part[j * rows : (j + 1) * rows]
        if c == 0:
            pl.semaphore_wait(barrier, ndev - 1)
        loop(ndp - 1, send_share(c))

    for copy in loads[1:]:
        copy.wait()
    line = lax.broadcasted_iota(jnp.int32, (rows, ncols), 0)

    def row_scale(ref):
        scale = jnp.full((rows, ncols), ref[0], F32)
        for r in range(1, rows):
            scale = jnp.where(line == r, ref[r], scale)
        return scale

    level1 = (code1[...].astype(F32) - 7.5) / 7.5
    old1[...] = 0.9 * (level1 * jnp.minimum(row_scale(rows1_ref), cols1[...]))
    level2 = (code2[...].astype(F32) + 1.0) / 16.0
    old2[...] = 0.95 * (level2 * level2 * jnp.minimum(row_scale(rows2_ref), cols2[...]))
    steps = jnp.full((1, 128), step_ref[0], jnp.int32).astype(F32)
    fix1 = (1.0 - jnp.exp(steps * jnp.log(F32(0.9))))[:, :1]
    fix2 = (1.0 - jnp.exp(steps * jnp.log(F32(0.95))))[:, :1]

    def wait_all(ref, count, which):
        blocks = ref.at[pl.ds(0, count)]
        pltpu.make_async_copy(blocks, blocks, which).wait()

    wait_all(grads, ndp - 1, recv_sem.at[0])
    gradient = share[dp]
    if ndp <= 32:
        for k in range(ndp - 1):
            gradient += grads[k]
    else:
        gradient = lax.fori_loop(0, ndp - 1, lambda k, total: total + grads[k], gradient)

    lanes = jnp.sum(gradient * gradient, axis=0, keepdims=True)
    total = lanes[:, :128]
    for b in range(1, ncols // 128):
        total += lanes[:, b * 128 : (b + 1) * 128]
    square[0] = total

    def send_square(k):
        pltpu.make_async_remote_copy(
            src_ref=square.at[0],
            dst_ref=squares.at[k],
            send_sem=send_sem.at[1],
            recv_sem=recv_sem.at[1],
            device_id=peer(k),
            device_id_type=MESH,
        ).start()

    loop(ndev - 1, send_square)
    wait_all(squares, ndev - 1, recv_sem.at[1])
    total = total + jnp.sum(squares[...], axis=0)
    norm = jnp.sqrt(jnp.sum(total, axis=1, keepdims=True))
    entries = rows * ncols * ndev
    clipf = jnp.minimum(1.0, 0.01 * jnp.sqrt(F32(entries)) / (norm + 1e-6))
    clipped = clipf * gradient

    new1 = old1[...] + 0.1 * clipped
    new2 = old2[...] + 0.05 * (clipped * clipped)
    abs1 = jnp.abs(new1)
    maxcol[0, 0:1] = jnp.max(abs1, axis=0, keepdims=True)
    maxcol[0, 1:2] = jnp.max(new2, axis=0, keepdims=True)

    def send_cols(k):
        pltpu.make_async_remote_copy(
            src_ref=maxcol.at[0],
            dst_ref=maxcols.at[k],
            send_sem=send_sem.at[2],
            recv_sem=recv_sem.at[2],
            device_id={"dp": lax.rem(dp + k + 1, ndp)},
            device_id_type=MESH,
        ).start()

    loop(ndp - 1, send_cols)

    maxrow[0, 0] = jnp.broadcast_to(jnp.max(abs1, axis=1, keepdims=True), (rows, 128))
    maxrow[0, 1] = jnp.broadcast_to(jnp.max(new2, axis=1, keepdims=True), (rows, 128))

    def send_rows(k):
        pltpu.make_async_remote_copy(
            src_ref=maxrow.at[0],
            dst_ref=maxrows.at[k],
            send_sem=send_sem.at[3],
            recv_sem=recv_sem.at[3],
            device_id={"mp": lax.rem(mp + k + 1, nmp)},
            device_id_type=MESH,
        ).start()

    loop(nmp - 1, send_rows)

    ratio = new1 / fix1 / (jnp.sqrt(new2 / fix2) + 1e-8)
    weights = master[...]
    weights = weights - 0.001 * (ratio + 0.1 * weights)
    params[dp] = weights.astype(jnp.bfloat16)

    def send_params(k):
        pltpu.make_async_remote_copy(
            src_ref=params.at[dp],
            dst_ref=params.at[dp],
            send_sem=send_sem.at[4],
            recv_sem=recv_sem.at[4],
            device_id={"dp": lax.rem(dp + k + 1, ndp)},
            device_id_type=MESH,
        ).start()

    loop(ndp - 1, send_params)
    master_out[...] = weights
    ratio_out[...] = ratio

    wait_all(maxrows, nmp - 1, recv_sem.at[3])
    toprow = maxrow[0]
    for k in range(nmp - 1):
        toprow = jnp.maximum(toprow, maxrows[k])
    rows_out[...] = toprow
    wait_all(maxcols, ndp - 1, recv_sem.at[2])
    topcol = maxcol[0]
    if ndp <= 32:
        for k in range(ndp - 1):
            topcol = jnp.maximum(topcol, maxcols[k])
    else:
        topcol = lax.fori_loop(
            0, ndp - 1, lambda k, top: jnp.maximum(top, maxcols[k]), topcol
        )
    newcols1_out[...] = topcol[0:1]
    newcols2_out[...] = topcol[1:2]
    scaled1_out[...] = new1 / (jnp.minimum(toprow[0][:, :1], topcol[0:1]) + 1e-8)
    scaled2_out[...] = new2 / (jnp.minimum(toprow[1][:, :1], topcol[1:2]) + 1e-8)

    wait_all(params, ndp - 1, recv_sem.at[4])
    params_out[...] = params[...]

    wait_all(grads, ndp - 1, send_sem.at[0])
    wait_all(squares, ndev - 1, send_sem.at[1])
    wait_all(maxcols, ndp - 1, send_sem.at[2])
    wait_all(maxrows, nmp - 1, send_sem.at[3])
    wait_all(params, ndp - 1, send_sem.at[4])


def shards(
    ndp,
    nmp,
    hidden_input,
    output_cotangent,
    master_weights,
    first_codes,
    second_codes,
    first_rows,
    first_cols,
    second_rows,
    second_cols,
    step_count,
):
    rows, ncols = master_weights.shape
    tokens, width = hidden_input.shape
    chunks = 4
    anyspace = pl.BlockSpec(memory_space=pl.ANY)
    smem = pl.BlockSpec(memory_space=pltpu.SMEM)
    vmem = pl.BlockSpec(memory_space=pltpu.VMEM)
    whole = jax.ShapeDtypeStruct((rows, ncols), F32)
    line = jax.ShapeDtypeStruct((1, ncols), F32)
    outs = pl.pallas_call(
        functools.partial(kernel, ndp, nmp, chunks),
        out_shape=(
            whole,
            whole,
            jax.ShapeDtypeStruct((ndp, rows, ncols), jnp.bfloat16),
            whole,
            whole,
            jax.ShapeDtypeStruct((2, rows, 128), F32),
            line,
            line,
        ),
        in_specs=[anyspace] * 7 + [smem] * 3,
        out_specs=[vmem] * 8,
        scratch_shapes=[
            pltpu.VMEM((width, tokens), jnp.bfloat16),
            pltpu.VMEM((chunks, tokens, ncols // chunks), jnp.bfloat16),
            pltpu.VMEM((rows, ncols), F32),
            pltpu.VMEM((rows, ncols), jnp.int32),
            pltpu.VMEM((rows, ncols), jnp.int32),
            pltpu.VMEM((1, ncols), F32),
            pltpu.VMEM((1, ncols), F32),
            pltpu.VMEM((ndp, rows, ncols), F32),
            pltpu.VMEM((ndp - 1, rows, ncols), F32),
            pltpu.VMEM((1, 1, 128), F32),
            pltpu.VMEM((ndp * nmp - 1, 1, 128), F32),
            pltpu.VMEM((ndp, rows, ncols), jnp.bfloat16),
            pltpu.VMEM((1, 2, ncols), F32),
            pltpu.VMEM((ndp - 1, 2, ncols), F32),
            pltpu.VMEM((1, 2, rows, 128), F32),
            pltpu.VMEM((nmp - 1, 2, rows, 128), F32),
            pltpu.VMEM((rows, ncols), F32),
            pltpu.VMEM((rows, ncols), F32),
            pltpu.SemaphoreType.DMA((6,)),
            pltpu.SemaphoreType.DMA((chunks,)),
            pltpu.SemaphoreType.DMA((5,)),
            pltpu.SemaphoreType.DMA((5,)),
        ],
        compiler_params=pltpu.CompilerParams(
            collective_id=0, has_side_effects=True, vmem_limit_bytes=60 * 1024 * 1024
        ),
    )(
        hidden_input.T,
        output_cotangent,
        master_weights,
        first_codes,
        second_codes,
        first_cols.reshape(1, ncols),
        second_cols.reshape(1, ncols),
        first_rows,
        second_rows,
        step_count.reshape(1),
    )
    master, ratio, params, scaled1, scaled2, toprows, cols1, cols2 = outs
    return (
        master,
        ratio,
        params.reshape(ndp * rows, ncols),
        scaled1,
        scaled2,
        toprows[0, :, 0],
        cols1.reshape(ncols),
        toprows[1, :, 0],
        cols2.reshape(ncols),
    )


def solution(mesh):
    return jax.shard_map(
        functools.partial(shards, mesh.shape["dp"], mesh.shape["mp"]),
        mesh=mesh,
        in_specs=(
            P("dp", None),
            P("dp", "mp"),
            P("dp", "mp"),
            P("dp", "mp"),
            P("dp", "mp"),
            P("dp"),
            P("mp"),
            P("dp"),
            P("mp"),
            P(),
        ),
        out_specs=(
            P("dp", "mp"),
            P("dp", "mp"),
            P(None, "mp"),
            P("dp", "mp"),
            P("dp", "mp"),
            P("dp"),
            P("mp"),
            P("dp"),
            P("mp"),
        ),
        check_vma=False,
    )
```

```python
import functools

import jax
import jax.numpy as jnp
from jax import lax
from jax.experimental import pallas as pl
from jax.experimental.pallas import tpu as pltpu
from jax.sharding import PartitionSpec as P

MESH = pl.DeviceIdType.MESH
F32 = jnp.float32


SUB = 8
LANES = 128


def kernel(
    ndp,
    nmp,
    loads_per_part,
    hidden_hbm,
    cot_hbm,
    master_hbm,
    code1_hbm,
    code2_hbm,
    cols1_hbm,
    cols2_hbm,
    rows1_hbm,
    rows2_hbm,
    step_hbm,
    master_out,
    ratio_out,
    params_out,
    scaled1_out,
    scaled2_out,
    rows_out,
    cols_out,
    hidden,
    cot,
    master,
    code1,
    code2,
    cols1,
    cols2,
    rows1,
    rows2,
    step_count,
    share,
    grads,
    square,
    squares,
    params,
    maxcol,
    maxcols,
    maxrow,
    maxrows,
    old1,
    old2,
    weights,
    in_sem,
    cot_sem,
    send_sem,
    recv_sem,
):
    dp = lax.axis_index("dp")
    mp = lax.axis_index("mp")
    ndev = ndp * nmp
    flat = dp * nmp + mp
    rows, ncols = master.shape
    parts = ncols // (SUB * LANES)
    deep = rows * SUB
    pieces = parts * loads_per_part
    width = ncols // pieces

    def loop(count, body):
        def step(i, carry):
            body(i)
            return carry

        lax.fori_loop(0, count, step, 0, unroll=count <= 32)

    loads = [
        pltpu.make_async_copy(src, dst, in_sem.at[i])
        for i, (src, dst) in enumerate(
            (
                (hidden_hbm, hidden),
                (code1_hbm, code1),
                (code2_hbm, code2),
                (cols1_hbm, cols1),
                (cols2_hbm, cols2),
                (master_hbm, master),
                (rows1_hbm, rows1),
                (rows2_hbm, rows2),
                (step_hbm, step_count),
            )
        )
    ]
    cot_loads = [
        pltpu.make_async_copy(
            cot_hbm.at[:, pl.ds(c * width, width)], cot.at[c], cot_sem.at[c]
        )
        for c in range(pieces)
    ]
    loads[0].start()
    for copy in cot_loads:
        copy.start()
    for copy in loads[1:]:
        copy.start()

    def peer(k):
        other = lax.rem(flat + k + 1, ndev)
        return {"dp": lax.div(other, nmp), "mp": lax.rem(other, nmp)}

    barrier = pltpu.get_barrier_semaphore()
    loop(
        ndev - 1,
        lambda k: pl.semaphore_signal(
            barrier, inc=1, device_id=peer(k), device_id_type=MESH
        ),
    )

    def send_share(p):
        def body(k):
            to = lax.rem(dp + k + 1, ndp)
            pltpu.make_async_remote_copy(
                src_ref=share.at[p, pl.ds(pl.multiple_of(to * deep, SUB), deep)],
                dst_ref=grads.at[k, pl.ds(p * deep, deep)],
                send_sem=send_sem.at[0],
                recv_sem=recv_sem.at[0],
                device_id={"dp": to},
                device_id_type=MESH,
            ).start()

        return body

    loads[0].wait()
    per_piece = width // LANES
    for c in range(pieces):
        cot_loads[c].wait()
        term = jnp.dot(hidden[...], cot[c], preferred_element_type=F32)
        p = c // loads_per_part
        for i in range(per_piece):
            sub = (c % loads_per_part) * per_piece + i
            share[p, pl.ds(sub, ndp * rows, stride=SUB), :] = term[
                :, i * LANES : (i + 1) * LANES
            ]
        if c == loads_per_part - 1:
            pl.semaphore_wait(barrier, ndev - 1)
        if c % loads_per_part == loads_per_part - 1:
            loop(ndp - 1, send_share(p))

    for copy in loads[1:]:
        copy.wait()

    def dense(value, ref):
        for b in range(ncols // LANES):
            at = (b // SUB) * deep + b % SUB
            ref[pl.ds(at, rows, stride=SUB), :] = value[:, b * LANES : (b + 1) * LANES]

    dense(code1[...].astype(F32), old1)
    dense(code2[...].astype(F32), old2)
    dense(master[...], weights)

    def scale(row_of, cols):
        tiles = []
        for p in range(parts):
            for r in range(rows):
                tiles.append(jnp.minimum(row_of(r), cols[p * SUB : (p + 1) * SUB]))
        return jnp.concatenate(tiles, axis=0)

    def tile(x, p, r):
        at = p * deep + r * SUB
        return x[at : at + SUB]

    level1 = (old1[...] - 7.5) / 7.5
    moment1 = 0.9 * (level1 * scale(lambda r: rows1[:, r : r + 1], cols1[...]))
    level2 = (old2[...] + 1.0) / 16.0
    moment2 = 0.95 * (level2 * level2 * scale(lambda r: rows2[:, r : r + 1], cols2[...]))
    steps = step_count[...].astype(F32)
    fix1 = 1.0 - jnp.exp(steps * jnp.log(F32(0.9)))
    fix2 = 1.0 - jnp.exp(steps * jnp.log(F32(0.95)))

    def wait_all(ref, count, which):
        blocks = ref.at[pl.ds(0, count)]
        pltpu.make_async_copy(blocks, blocks, which).wait()

    def fold(fn, first, ref, count):
        if count <= 32:
            for k in range(count):
                first = fn(first, ref[k])
            return first
        return lax.fori_loop(0, count, lambda k, x: fn(x, ref[k]), first)

    mine = pl.ds(pl.multiple_of(dp * deep, SUB), deep)
    gradient = jnp.concatenate([share[p, mine, :] for p in range(parts)], axis=0)
    wait_all(grads, ndp - 1, recv_sem.at[0])
    gradient = fold(jnp.add, gradient, grads, ndp - 1)

    lanes = jnp.sum(gradient * gradient, axis=0, keepdims=True)
    square[0] = lanes

    def send_square(k):
        pltpu.make_async_remote_copy(
            src_ref=square.at[0],
            dst_ref=squares.at[k],
            send_sem=send_sem.at[1],
            recv_sem=recv_sem.at[1],
            device_id=peer(k),
            device_id_type=MESH,
        ).start()

    loop(ndev - 1, send_square)
    wait_all(squares, ndev - 1, recv_sem.at[1])
    lanes = lanes + jnp.sum(squares[...], axis=0)
    norm = jnp.sqrt(jnp.sum(lanes, axis=1, keepdims=True))
    entries = rows * ncols * ndev
    clipf = jnp.minimum(1.0, 0.01 * jnp.sqrt(F32(entries)) / (norm + 1e-6))
    clipped = clipf * gradient

    new1 = moment1 + 0.1 * clipped
    new2 = moment2 + 0.05 * (clipped * clipped)
    abs1 = jnp.abs(new1)

    def over_rows(x):
        tops = []
        for p in range(parts):
            top = tile(x, p, 0)
            for r in range(1, rows):
                top = jnp.maximum(top, tile(x, p, r))
            tops.append(top)
        return jnp.concatenate(tops, axis=0)

    maxcol[0, 0] = over_rows(abs1)
    maxcol[0, 1] = over_rows(new2)

    def send_cols(k):
        pltpu.make_async_remote_copy(
            src_ref=maxcol.at[0],
            dst_ref=maxcols.at[k],
            send_sem=send_sem.at[2],
            recv_sem=recv_sem.at[2],
            device_id={"dp": lax.rem(dp + k + 1, ndp)},
            device_id_type=MESH,
        ).start()

    loop(ndp - 1, send_cols)

    ratio = new1 / fix1 / (jnp.sqrt(new2 / fix2) + 1e-8)
    old_weights = weights[...]
    new_weights = old_weights - 0.001 * (ratio + 0.1 * old_weights)
    params[dp] = new_weights.astype(jnp.bfloat16)

    def send_params(k):
        pltpu.make_async_remote_copy(
            src_ref=params.at[dp],
            dst_ref=params.at[dp],
            send_sem=send_sem.at[4],
            recv_sem=recv_sem.at[4],
            device_id={"dp": lax.rem(dp + k + 1, ndp)},
            device_id_type=MESH,
        ).start()

    loop(ndp - 1, send_params)

    def over_cols(x):
        tops = []
        for r in range(rows):
            top = tile(x, 0, r)
            for p in range(1, parts):
                top = jnp.maximum(top, tile(x, p, r))
            tops.append(jnp.max(top, axis=0, keepdims=True))
        return tops

    tops = jnp.concatenate(over_cols(abs1) + over_cols(new2), axis=0)
    maxrow[0] = jnp.broadcast_to(jnp.max(tops, axis=1, keepdims=True), tops.shape)

    def send_rows(k):
        pltpu.make_async_remote_copy(
            src_ref=maxrow.at[0],
            dst_ref=maxrows.at[k],
            send_sem=send_sem.at[3],
            recv_sem=recv_sem.at[3],
            device_id={"mp": lax.rem(mp + k + 1, nmp)},
            device_id_type=MESH,
        ).start()

    loop(nmp - 1, send_rows)
    master_out[...] = new_weights
    ratio_out[...] = ratio

    wait_all(maxrows, nmp - 1, recv_sem.at[3])
    toprow = fold(jnp.maximum, maxrow[0], maxrows, nmp - 1)
    rows_out[...] = toprow
    wait_all(maxcols, ndp - 1, recv_sem.at[2])
    topcol = fold(jnp.maximum, maxcol[0], maxcols, ndp - 1)
    cols_out[...] = topcol
    scaled1_out[...] = new1 / (scale(lambda r: toprow[r : r + 1], topcol[0]) + 1e-8)
    scaled2_out[...] = new2 / (
        scale(lambda r: toprow[rows + r : rows + r + 1], topcol[1]) + 1e-8
    )

    wait_all(params, ndp - 1, recv_sem.at[4])
    params_out[...] = params[...]

    wait_all(grads, ndp - 1, send_sem.at[0])
    wait_all(squares, ndev - 1, send_sem.at[1])
    wait_all(maxcols, ndp - 1, send_sem.at[2])
    wait_all(maxrows, nmp - 1, send_sem.at[3])
    wait_all(params, ndp - 1, send_sem.at[4])


def unpack(
    master,
    ratio,
    params,
    scaled1,
    scaled2,
    toprows,
    topcols,
    master_out,
    ratio_out,
    params_out,
    scaled1_out,
    scaled2_out,
    rows1_out,
    cols1_out,
    rows2_out,
    cols2_out,
    wide,
):
    rows, ncols = master_out.shape
    ndp = params.shape[0]
    parts = ncols // (SUB * LANES)
    deep = rows * SUB

    cols1_out[...] = topcols[0]
    cols2_out[...] = topcols[1]
    for r in range(rows):
        rows1_out[r] = jnp.max(toprows[r : r + 1, :])
        rows2_out[r] = jnp.max(toprows[rows + r : rows + r + 1, :])
    for j in range(ndp):
        block = params[j].astype(F32)
        for p in range(parts):
            wide[p, j * deep : (j + 1) * deep] = block[p * deep : (p + 1) * deep]
    for b in range(ncols // LANES):
        p, sub = b // SUB, b % SUB
        cols = slice(b * LANES, (b + 1) * LANES)
        part = pl.ds(p * deep + sub, rows, stride=SUB)
        master_out[:, cols] = master[part, :]
        ratio_out[:, cols] = ratio[part, :]
        scaled1_out[:, cols] = scaled1[part, :]
        scaled2_out[:, cols] = scaled2[part, :]
        params_out[:, cols] = wide[p, pl.ds(sub, ndp * rows, stride=SUB), :].astype(
            jnp.bfloat16
        )


def shards(
    ndp,
    nmp,
    hidden_input,
    output_cotangent,
    master_weights,
    first_codes,
    second_codes,
    first_rows,
    first_cols,
    second_rows,
    second_cols,
    step_count,
):
    rows, ncols = master_weights.shape
    tokens, width = hidden_input.shape
    parts = ncols // (SUB * LANES)
    loads = 2
    height = parts * rows * SUB
    hbm = pl.BlockSpec(memory_space=pltpu.HBM)
    smem = pl.BlockSpec(memory_space=pltpu.SMEM)
    vmem = pl.BlockSpec(memory_space=pltpu.VMEM)
    whole = jax.ShapeDtypeStruct((rows, ncols), F32)
    block = (height, LANES)
    line = (parts * SUB, LANES)
    dense = pltpu.VMEM(block, F32)
    results = pl.pallas_call(
        functools.partial(kernel, ndp, nmp, loads),
        out_shape=(
            dense,
            dense,
            pltpu.VMEM((ndp, *block), jnp.bfloat16),
            dense,
            dense,
            pltpu.VMEM((2 * rows, LANES), F32),
            pltpu.VMEM((2, *line), F32),
        ),
        in_specs=[hbm] * 10,
        out_specs=[vmem] * 7,
        scratch_shapes=[
            pltpu.VMEM((width, tokens), jnp.bfloat16),
            pltpu.VMEM((parts * loads, tokens, ncols // (parts * loads)), jnp.bfloat16),
            pltpu.VMEM((rows, ncols), F32),
            pltpu.VMEM((rows, ncols), jnp.int32),
            pltpu.VMEM((rows, ncols), jnp.int32),
            pltpu.VMEM(line, F32),
            pltpu.VMEM(line, F32),
            pltpu.VMEM((1, rows), F32),
            pltpu.VMEM((1, rows), F32),
            pltpu.VMEM((1, 1), jnp.int32),
            pltpu.VMEM((parts, ndp * rows * SUB, LANES), F32),
            pltpu.VMEM((ndp - 1, *block), F32),
            pltpu.VMEM((1, 1, LANES), F32),
            pltpu.VMEM((ndp * nmp - 1, 1, LANES), F32),
            pltpu.VMEM((ndp, *block), jnp.bfloat16),
            pltpu.VMEM((1, 2, *line), F32),
            pltpu.VMEM((ndp - 1, 2, *line), F32),
            pltpu.VMEM((1, 2 * rows, LANES), F32),
            pltpu.VMEM((nmp - 1, 2 * rows, LANES), F32),
            pltpu.VMEM(block, F32),
            pltpu.VMEM(block, F32),
            pltpu.VMEM(block, F32),
            pltpu.SemaphoreType.DMA((9,)),
            pltpu.SemaphoreType.DMA((parts * loads,)),
            pltpu.SemaphoreType.DMA((5,)),
            pltpu.SemaphoreType.DMA((5,)),
        ],
        compiler_params=pltpu.CompilerParams(
            collective_id=0, has_side_effects=True, vmem_limit_bytes=60 * 1024 * 1024
        ),
    )(
        hidden_input.T,
        output_cotangent,
        master_weights,
        first_codes,
        second_codes,
        first_cols.reshape(line),
        second_cols.reshape(line),
        first_rows.reshape(1, rows),
        second_rows.reshape(1, rows),
        step_count.reshape(1, 1),
    )
    scales = jax.ShapeDtypeStruct((rows,), F32)
    cols = jax.ShapeDtypeStruct(line, F32)
    outs = pl.pallas_call(
        unpack,
        out_shape=(
            whole,
            whole,
            jax.ShapeDtypeStruct((ndp * rows, ncols), jnp.bfloat16),
            whole,
            whole,
            scales,
            cols,
            scales,
            cols,
        ),
        in_specs=[vmem] * 7,
        out_specs=[vmem] * 5 + [smem, vmem] * 2,
        scratch_shapes=[pltpu.VMEM((parts, ndp * rows * SUB, LANES), F32)],
        compiler_params=pltpu.CompilerParams(vmem_limit_bytes=40 * 1024 * 1024),
    )(*results)
    return (*outs[:6], outs[6].reshape(ncols), outs[7], outs[8].reshape(ncols))


def solution(mesh):
    return jax.shard_map(
        functools.partial(shards, mesh.shape["dp"], mesh.shape["mp"]),
        mesh=mesh,
        in_specs=(
            P("dp", None),
            P("dp", "mp"),
            P("dp", "mp"),
            P("dp", "mp"),
            P("dp", "mp"),
            P("dp"),
            P("mp"),
            P("dp"),
            P("mp"),
            P(),
        ),
        out_specs=(
            P("dp", "mp"),
            P("dp", "mp"),
            P(None, "mp"),
            P("dp", "mp"),
            P("dp", "mp"),
            P("dp"),
            P("mp"),
            P("dp"),
            P("mp"),
        ),
        check_vma=False,
    )
```

```python
import functools

import jax
import jax.numpy as jnp
from jax import lax
from jax.experimental import pallas as pl
from jax.experimental.pallas import tpu as pltpu
from jax.sharding import PartitionSpec as P

MESH = pl.DeviceIdType.MESH
F32 = jnp.float32


SUB = 8
LANES = 128


def kernel(
    ndp,
    nmp,
    loads_per_part,
    hidden_hbm,
    cot_hbm,
    master_hbm,
    code1_hbm,
    code2_hbm,
    cols1_hbm,
    cols2_hbm,
    rows1_hbm,
    rows2_hbm,
    step_hbm,
    master_out,
    ratio_out,
    params_out,
    scaled1_out,
    scaled2_out,
    rows_out,
    cols_out,
    hidden,
    cot,
    master,
    code1,
    code2,
    cols1,
    cols2,
    rows1,
    rows2,
    step_count,
    share,
    grads,
    square,
    squares,
    params,
    maxcol,
    maxcols,
    maxrow,
    maxrows,
    old1,
    old2,
    weights,
    in_sem,
    cot_sem,
    send_sem,
    recv_sem,
):
    dp = lax.axis_index("dp")
    mp = lax.axis_index("mp")
    ndev = ndp * nmp
    flat = dp * nmp + mp
    rows, ncols = master.shape
    parts = ncols // (SUB * LANES)
    deep = rows * SUB
    pieces = parts * loads_per_part
    width = ncols // pieces

    def loop(count, body):
        def step(i, carry):
            body(i)
            return carry

        lax.fori_loop(0, count, step, 0, unroll=count <= 32)

    loads = [
        pltpu.make_async_copy(src, dst, in_sem.at[i])
        for i, (src, dst) in enumerate(
            (
                (hidden_hbm, hidden),
                (code1_hbm, code1),
                (code2_hbm, code2),
                (cols1_hbm, cols1),
                (cols2_hbm, cols2),
                (master_hbm, master),
                (rows1_hbm, rows1),
                (rows2_hbm, rows2),
                (step_hbm, step_count),
            )
        )
    ]
    cot_loads = [
        pltpu.make_async_copy(
            cot_hbm.at[:, pl.ds(c * width, width)], cot.at[c], cot_sem.at[c]
        )
        for c in range(pieces)
    ]
    loads[0].start()
    for copy in cot_loads:
        copy.start()
    for copy in loads[1:]:
        copy.start()

    def peer(k):
        other = lax.rem(flat + k + 1, ndev)
        return {"dp": lax.div(other, nmp), "mp": lax.rem(other, nmp)}

    barrier = pltpu.get_barrier_semaphore()
    loop(
        ndev - 1,
        lambda k: pl.semaphore_signal(
            barrier, inc=1, device_id=peer(k), device_id_type=MESH
        ),
    )

    def send_share(p):
        def body(k):
            to = lax.rem(dp + k + 1, ndp)
            pltpu.make_async_remote_copy(
                src_ref=share.at[p, pl.ds(pl.multiple_of(to * deep, SUB), deep)],
                dst_ref=grads.at[k, pl.ds(p * deep, deep)],
                send_sem=send_sem.at[0],
                recv_sem=recv_sem.at[0],
                device_id={"dp": to},
                device_id_type=MESH,
            ).start()

        return body

    loads[0].wait()
    per_piece = width // LANES
    for c in range(pieces):
        cot_loads[c].wait()
        term = jnp.dot(hidden[...], cot[c], preferred_element_type=F32)
        p = c // loads_per_part
        for i in range(per_piece):
            sub = (c % loads_per_part) * per_piece + i
            share[p, pl.ds(sub, ndp * rows, stride=SUB), :] = term[
                :, i * LANES : (i + 1) * LANES
            ]
        if c == loads_per_part - 1:
            pl.semaphore_wait(barrier, ndev - 1)
        if c % loads_per_part == loads_per_part - 1:
            loop(ndp - 1, send_share(p))

    for copy in loads[1:]:
        copy.wait()

    def dense(value, ref):
        for b in range(ncols // LANES):
            at = (b // SUB) * deep + b % SUB
            ref[pl.ds(at, rows, stride=SUB), :] = value[:, b * LANES : (b + 1) * LANES]

    dense(code1[...].astype(F32), old1)
    dense(code2[...].astype(F32), old2)
    dense(master[...], weights)

    def scale(row_of, cols):
        tiles = []
        for p in range(parts):
            for r in range(rows):
                tiles.append(jnp.minimum(row_of(r), cols[p * SUB : (p + 1) * SUB]))
        return jnp.concatenate(tiles, axis=0)

    def tile(x, p, r):
        at = p * deep + r * SUB
        return x[at : at + SUB]

    level1 = (old1[...] - 7.5) / 7.5
    moment1 = 0.9 * (level1 * scale(lambda r: rows1[:, r : r + 1], cols1[...]))
    level2 = (old2[...] + 1.0) / 16.0
    moment2 = 0.95 * (level2 * level2 * scale(lambda r: rows2[:, r : r + 1], cols2[...]))
    steps = step_count[...].astype(F32)
    fix1 = 1.0 - jnp.exp(steps * jnp.log(F32(0.9)))
    fix2 = 1.0 - jnp.exp(steps * jnp.log(F32(0.95)))

    def wait_all(ref, count, which):
        blocks = ref.at[pl.ds(0, count)]
        pltpu.make_async_copy(blocks, blocks, which).wait()

    def fold(fn, first, ref, count):
        if count <= 32:
            for k in range(count):
                first = fn(first, ref[k])
            return first
        return lax.fori_loop(0, count, lambda k, x: fn(x, ref[k]), first)

    mine = pl.ds(pl.multiple_of(dp * deep, SUB), deep)
    gradient = jnp.concatenate([share[p, mine, :] for p in range(parts)], axis=0)
    wait_all(grads, ndp - 1, recv_sem.at[0])
    gradient = fold(jnp.add, gradient, grads, ndp - 1)

    lanes = jnp.sum(gradient * gradient, axis=0, keepdims=True)
    square[0] = lanes

    def send_square(k):
        pltpu.make_async_remote_copy(
            src_ref=square.at[0],
            dst_ref=squares.at[k],
            send_sem=send_sem.at[1],
            recv_sem=recv_sem.at[1],
            device_id=peer(k),
            device_id_type=MESH,
        ).start()

    loop(ndev - 1, send_square)
    wait_all(squares, ndev - 1, recv_sem.at[1])
    lanes = lanes + jnp.sum(squares[...], axis=0)
    norm = jnp.sqrt(jnp.sum(lanes, axis=1, keepdims=True))
    entries = rows * ncols * ndev
    clipf = jnp.minimum(1.0, 0.01 * jnp.sqrt(F32(entries)) / (norm + 1e-6))
    clipped = clipf * gradient

    new1 = moment1 + 0.1 * clipped
    new2 = moment2 + 0.05 * (clipped * clipped)
    abs1 = jnp.abs(new1)

    def over_rows(x):
        tops = []
        for p in range(parts):
            top = tile(x, p, 0)
            for r in range(1, rows):
                top = jnp.maximum(top, tile(x, p, r))
            tops.append(top)
        return jnp.concatenate(tops, axis=0)

    maxcol[0, 0] = over_rows(abs1)
    maxcol[0, 1] = over_rows(new2)

    pair = pltpu.make_async_remote_copy(
        src_ref=maxcol.at[0],
        dst_ref=maxcol.at[1],
        send_sem=send_sem.at[5],
        recv_sem=recv_sem.at[5],
        device_id={"dp": dp + 1 - 2 * lax.rem(dp, 2)},
        device_id_type=MESH,
    )
    pair.start()

    ratio = new1 / fix1 / (jnp.sqrt(new2 / fix2) + 1e-8)
    old_weights = weights[...]
    new_weights = old_weights - 0.001 * (ratio + 0.1 * old_weights)
    params[dp] = new_weights.astype(jnp.bfloat16)

    def send_params(k):
        pltpu.make_async_remote_copy(
            src_ref=params.at[dp],
            dst_ref=params.at[dp],
            send_sem=send_sem.at[4],
            recv_sem=recv_sem.at[4],
            device_id={"dp": lax.rem(dp + k + 1, ndp)},
            device_id_type=MESH,
        ).start()

    loop(ndp - 1, send_params)

    def over_cols(x):
        tops = []
        for r in range(rows):
            top = tile(x, 0, r)
            for p in range(1, parts):
                top = jnp.maximum(top, tile(x, p, r))
            tops.append(jnp.max(top, axis=0, keepdims=True))
        return tops

    tops = jnp.concatenate(over_cols(abs1) + over_cols(new2), axis=0)
    maxrow[0] = jnp.broadcast_to(jnp.max(tops, axis=1, keepdims=True), tops.shape)

    def send_rows(k):
        pltpu.make_async_remote_copy(
            src_ref=maxrow.at[0],
            dst_ref=maxrows.at[k],
            send_sem=send_sem.at[3],
            recv_sem=recv_sem.at[3],
            device_id={"mp": lax.rem(mp + k + 1, nmp)},
            device_id_type=MESH,
        ).start()

    loop(nmp - 1, send_rows)

    def send_cols(k):
        pltpu.make_async_remote_copy(
            src_ref=maxcol.at[2],
            dst_ref=maxcols.at[k],
            send_sem=send_sem.at[2],
            recv_sem=recv_sem.at[2],
            device_id={"dp": lax.rem(dp + 2 * (k + 1), ndp)},
            device_id_type=MESH,
        ).start()

    pair.wait_recv()
    maxcol[2] = jnp.maximum(maxcol[0], maxcol[1])
    loop(ndp // 2 - 1, send_cols)
    master_out[...] = new_weights
    ratio_out[...] = ratio

    wait_all(maxrows, nmp - 1, recv_sem.at[3])
    toprow = fold(jnp.maximum, maxrow[0], maxrows, nmp - 1)
    rows_out[...] = toprow
    wait_all(maxcols, ndp // 2 - 1, recv_sem.at[2])
    topcol = fold(jnp.maximum, maxcol[2], maxcols, ndp // 2 - 1)
    cols_out[...] = topcol
    scaled1_out[...] = new1 / (scale(lambda r: toprow[r : r + 1], topcol[0]) + 1e-8)
    scaled2_out[...] = new2 / (
        scale(lambda r: toprow[rows + r : rows + r + 1], topcol[1]) + 1e-8
    )

    wait_all(params, ndp - 1, recv_sem.at[4])
    params_out[...] = params[...]

    wait_all(grads, ndp - 1, send_sem.at[0])
    wait_all(squares, ndev - 1, send_sem.at[1])
    pair.wait_send()
    wait_all(maxcols, ndp // 2 - 1, send_sem.at[2])
    wait_all(maxrows, nmp - 1, send_sem.at[3])
    wait_all(params, ndp - 1, send_sem.at[4])


def unpack(
    master,
    ratio,
    params,
    scaled1,
    scaled2,
    toprows,
    topcols,
    master_out,
    ratio_out,
    params_out,
    scaled1_out,
    scaled2_out,
    rows1_out,
    cols1_out,
    rows2_out,
    cols2_out,
    wide,
):
    rows, ncols = master_out.shape
    ndp = params.shape[0]
    parts = ncols // (SUB * LANES)
    deep = rows * SUB

    cols1_out[...] = topcols[0]
    cols2_out[...] = topcols[1]
    for r in range(rows):
        rows1_out[r] = jnp.max(toprows[r : r + 1, :])
        rows2_out[r] = jnp.max(toprows[rows + r : rows + r + 1, :])
    for j in range(ndp):
        block = params[j].astype(F32)
        for p in range(parts):
            wide[p, j * deep : (j + 1) * deep] = block[p * deep : (p + 1) * deep]
    for b in range(ncols // LANES):
        p, sub = b // SUB, b % SUB
        cols = slice(b * LANES, (b + 1) * LANES)
        part = pl.ds(p * deep + sub, rows, stride=SUB)
        master_out[:, cols] = master[part, :]
        ratio_out[:, cols] = ratio[part, :]
        scaled1_out[:, cols] = scaled1[part, :]
        scaled2_out[:, cols] = scaled2[part, :]
        params_out[:, cols] = wide[p, pl.ds(sub, ndp * rows, stride=SUB), :].astype(
            jnp.bfloat16
        )


def shards(
    ndp,
    nmp,
    hidden_input,
    output_cotangent,
    master_weights,
    first_codes,
    second_codes,
    first_rows,
    first_cols,
    second_rows,
    second_cols,
    step_count,
):
    rows, ncols = master_weights.shape
    tokens, width = hidden_input.shape
    parts = ncols // (SUB * LANES)
    loads = 2
    height = parts * rows * SUB
    hbm = pl.BlockSpec(memory_space=pltpu.HBM)
    smem = pl.BlockSpec(memory_space=pltpu.SMEM)
    vmem = pl.BlockSpec(memory_space=pltpu.VMEM)
    whole = jax.ShapeDtypeStruct((rows, ncols), F32)
    block = (height, LANES)
    line = (parts * SUB, LANES)
    dense = pltpu.VMEM(block, F32)
    results = pl.pallas_call(
        functools.partial(kernel, ndp, nmp, loads),
        out_shape=(
            dense,
            dense,
            pltpu.VMEM((ndp, *block), jnp.bfloat16),
            dense,
            dense,
            pltpu.VMEM((2 * rows, LANES), F32),
            pltpu.VMEM((2, *line), F32),
        ),
        in_specs=[hbm] * 10,
        out_specs=[vmem] * 7,
        scratch_shapes=[
            pltpu.VMEM((width, tokens), jnp.bfloat16),
            pltpu.VMEM((parts * loads, tokens, ncols // (parts * loads)), jnp.bfloat16),
            pltpu.VMEM((rows, ncols), F32),
            pltpu.VMEM((rows, ncols), jnp.int32),
            pltpu.VMEM((rows, ncols), jnp.int32),
            pltpu.VMEM(line, F32),
            pltpu.VMEM(line, F32),
            pltpu.VMEM((1, rows), F32),
            pltpu.VMEM((1, rows), F32),
            pltpu.VMEM((1, 1), jnp.int32),
            pltpu.VMEM((parts, ndp * rows * SUB, LANES), F32),
            pltpu.VMEM((ndp - 1, *block), F32),
            pltpu.VMEM((1, 1, LANES), F32),
            pltpu.VMEM((ndp * nmp - 1, 1, LANES), F32),
            pltpu.VMEM((ndp, *block), jnp.bfloat16),
            pltpu.VMEM((3, 2, *line), F32),
            pltpu.VMEM((ndp // 2 - 1, 2, *line), F32),
            pltpu.VMEM((1, 2 * rows, LANES), F32),
            pltpu.VMEM((nmp - 1, 2 * rows, LANES), F32),
            pltpu.VMEM(block, F32),
            pltpu.VMEM(block, F32),
            pltpu.VMEM(block, F32),
            pltpu.SemaphoreType.DMA((9,)),
            pltpu.SemaphoreType.DMA((parts * loads,)),
            pltpu.SemaphoreType.DMA((6,)),
            pltpu.SemaphoreType.DMA((6,)),
        ],
        compiler_params=pltpu.CompilerParams(
            collective_id=0, has_side_effects=True, vmem_limit_bytes=60 * 1024 * 1024
        ),
    )(
        hidden_input.T,
        output_cotangent,
        master_weights,
        first_codes,
        second_codes,
        first_cols.reshape(line),
        second_cols.reshape(line),
        first_rows.reshape(1, rows),
        second_rows.reshape(1, rows),
        step_count.reshape(1, 1),
    )
    scales = jax.ShapeDtypeStruct((rows,), F32)
    cols = jax.ShapeDtypeStruct(line, F32)
    outs = pl.pallas_call(
        unpack,
        out_shape=(
            whole,
            whole,
            jax.ShapeDtypeStruct((ndp * rows, ncols), jnp.bfloat16),
            whole,
            whole,
            scales,
            cols,
            scales,
            cols,
        ),
        in_specs=[vmem] * 7,
        out_specs=[vmem] * 5 + [smem, vmem] * 2,
        scratch_shapes=[pltpu.VMEM((parts, ndp * rows * SUB, LANES), F32)],
        compiler_params=pltpu.CompilerParams(vmem_limit_bytes=40 * 1024 * 1024),
    )(*results)
    return (*outs[:6], outs[6].reshape(ncols), outs[7], outs[8].reshape(ncols))


def solution(mesh):
    return jax.shard_map(
        functools.partial(shards, mesh.shape["dp"], mesh.shape["mp"]),
        mesh=mesh,
        in_specs=(
            P("dp", None),
            P("dp", "mp"),
            P("dp", "mp"),
            P("dp", "mp"),
            P("dp", "mp"),
            P("dp"),
            P("mp"),
            P("dp"),
            P("mp"),
            P(),
        ),
        out_specs=(
            P("dp", "mp"),
            P("dp", "mp"),
            P(None, "mp"),
            P("dp", "mp"),
            P("dp", "mp"),
            P("dp"),
            P("mp"),
            P("dp"),
            P("mp"),
        ),
        check_vma=False,
    )
```

```python
import functools

import jax
import jax.numpy as jnp
from jax import lax
from jax.experimental import pallas as pl
from jax.experimental.pallas import tpu as pltpu
from jax.sharding import PartitionSpec as P

MESH = pl.DeviceIdType.MESH
F32 = jnp.float32


SUB = 8
LANES = 128


def kernel(
    ndp,
    nmp,
    loads_per_part,
    hidden_hbm,
    cot_hbm,
    master_hbm,
    code1_hbm,
    code2_hbm,
    cols1_hbm,
    cols2_hbm,
    rows1_hbm,
    rows2_hbm,
    step_hbm,
    master_out,
    ratio_out,
    params_out,
    scaled1_out,
    scaled2_out,
    rows_out,
    cols_out,
    hidden,
    cot,
    master,
    code1,
    code2,
    cols1,
    cols2,
    rows1,
    rows2,
    step_count,
    share,
    grads,
    square,
    squares,
    params,
    maxcol,
    maxcols,
    maxrow,
    maxrows,
    old1,
    old2,
    weights,
    in_sem,
    cot_sem,
    send_sem,
    recv_sem,
):
    dp = lax.axis_index("dp")
    mp = lax.axis_index("mp")
    ndev = ndp * nmp
    flat = dp * nmp + mp
    rows, ncols = master.shape
    parts = ncols // (SUB * LANES)
    deep = rows * SUB
    pieces = parts * loads_per_part
    width = ncols // pieces

    def loop(count, body):
        def step(i, carry):
            body(i)
            return carry

        lax.fori_loop(0, count, step, 0, unroll=count <= 32)

    loads = [
        pltpu.make_async_copy(src, dst, in_sem.at[i])
        for i, (src, dst) in enumerate(
            (
                (hidden_hbm, hidden),
                (code1_hbm, code1),
                (code2_hbm, code2),
                (cols1_hbm, cols1),
                (cols2_hbm, cols2),
                (master_hbm, master),
                (rows1_hbm, rows1),
                (rows2_hbm, rows2),
                (step_hbm, step_count),
            )
        )
    ]
    cot_loads = [
        pltpu.make_async_copy(
            cot_hbm.at[:, pl.ds(c * width, width)], cot.at[c], cot_sem.at[c]
        )
        for c in range(pieces)
    ]
    def peer(k):
        other = lax.rem(flat + k + 1, ndev)
        return {"dp": lax.div(other, nmp), "mp": lax.rem(other, nmp)}

    barrier = pltpu.get_barrier_semaphore()
    loop(
        ndev - 1,
        lambda k: pl.semaphore_signal(
            barrier, inc=1, device_id=peer(k), device_id_type=MESH
        ),
    )

    loads[0].start()
    for copy in cot_loads:
        copy.start()
    for copy in loads[1:]:
        copy.start()

    def send_share(p):
        def body(k):
            to = lax.rem(dp + k + 1, ndp)
            pltpu.make_async_remote_copy(
                src_ref=share.at[p, pl.ds(pl.multiple_of(to * deep, SUB), deep)],
                dst_ref=grads.at[k, pl.ds(p * deep, deep)],
                send_sem=send_sem.at[0],
                recv_sem=recv_sem.at[0],
                device_id={"dp": to},
                device_id_type=MESH,
            ).start()

        return body

    loads[0].wait()
    per_piece = width // LANES
    for c in range(pieces):
        cot_loads[c].wait()
        term = jnp.dot(hidden[...], cot[c], preferred_element_type=F32)
        p = c // loads_per_part
        for i in range(per_piece):
            sub = (c % loads_per_part) * per_piece + i
            share[p, pl.ds(sub, ndp * rows, stride=SUB), :] = term[
                :, i * LANES : (i + 1) * LANES
            ]
        if c == loads_per_part - 1:
            pl.semaphore_wait(barrier, ndev - 1)
        if c % loads_per_part == loads_per_part - 1:
            loop(ndp - 1, send_share(p))

    for copy in loads[1:]:
        copy.wait()

    def dense(value, ref):
        for b in range(ncols // LANES):
            at = (b // SUB) * deep + b % SUB
            ref[pl.ds(at, rows, stride=SUB), :] = value[:, b * LANES : (b + 1) * LANES]

    dense(code1[...].astype(F32), old1)
    dense(code2[...].astype(F32), old2)
    dense(master[...], weights)

    def scale(row_of, cols):
        tiles = []
        for p in range(parts):
            for r in range(rows):
                tiles.append(jnp.minimum(row_of(r), cols[p * SUB : (p + 1) * SUB]))
        return jnp.concatenate(tiles, axis=0)

    def tile(x, p, r):
        at = p * deep + r * SUB
        return x[at : at + SUB]

    level1 = (old1[...] - 7.5) / 7.5
    moment1 = 0.9 * (level1 * scale(lambda r: rows1[:, r : r + 1], cols1[...]))
    level2 = (old2[...] + 1.0) / 16.0
    moment2 = 0.95 * (level2 * level2 * scale(lambda r: rows2[:, r : r + 1], cols2[...]))
    steps = step_count[...].astype(F32)
    fix1 = 1.0 - jnp.exp(steps * jnp.log(F32(0.9)))
    fix2 = 1.0 - jnp.exp(steps * jnp.log(F32(0.95)))

    def wait_all(ref, count, which):
        blocks = ref.at[pl.ds(0, count)]
        pltpu.make_async_copy(blocks, blocks, which).wait()

    def fold(fn, first, ref, count):
        if count <= 32:
            for k in range(count):
                first = fn(first, ref[k])
            return first
        return lax.fori_loop(0, count, lambda k, x: fn(x, ref[k]), first)

    mine = pl.ds(pl.multiple_of(dp * deep, SUB), deep)
    gradient = jnp.concatenate([share[p, mine, :] for p in range(parts)], axis=0)
    wait_all(grads, ndp - 1, recv_sem.at[0])
    gradient = fold(jnp.add, gradient, grads, ndp - 1)

    lanes = jnp.sum(gradient * gradient, axis=0, keepdims=True)
    square[0] = lanes

    def send_square(k):
        pltpu.make_async_remote_copy(
            src_ref=square.at[0],
            dst_ref=squares.at[ndev - 2 - k],
            send_sem=send_sem.at[1],
            recv_sem=recv_sem.at[1],
            device_id=peer(ndev - 2 - k),
            device_id_type=MESH,
        ).start()

    loop(ndev - 1, send_square)
    wait_all(squares, ndev - 1, recv_sem.at[1])
    lanes = lanes + jnp.sum(squares[...], axis=0)
    norm = jnp.sqrt(jnp.sum(lanes, axis=1, keepdims=True))
    entries = rows * ncols * ndev
    clipf = jnp.minimum(1.0, 0.01 * jnp.sqrt(F32(entries)) / (norm + 1e-6))
    clipped = clipf * gradient

    new1 = moment1 + 0.1 * clipped
    new2 = moment2 + 0.05 * (clipped * clipped)
    abs1 = jnp.abs(new1)

    def over_rows(x):
        tops = []
        for p in range(parts):
            top = tile(x, p, 0)
            for r in range(1, rows):
                top = jnp.maximum(top, tile(x, p, r))
            tops.append(top)
        return jnp.concatenate(tops, axis=0)

    maxcol[0, 0] = over_rows(abs1)
    maxcol[0, 1] = over_rows(new2)

    pair = pltpu.make_async_remote_copy(
        src_ref=maxcol.at[0],
        dst_ref=maxcol.at[1],
        send_sem=send_sem.at[5],
        recv_sem=recv_sem.at[5],
        device_id={"dp": dp + 1 - 2 * lax.rem(dp, 2)},
        device_id_type=MESH,
    )
    pair.start()

    def over_cols(x):
        tops = []
        for r in range(rows):
            top = tile(x, 0, r)
            for p in range(1, parts):
                top = jnp.maximum(top, tile(x, p, r))
            tops.append(jnp.max(top, axis=0, keepdims=True))
        return tops

    tops = jnp.concatenate(over_cols(abs1) + over_cols(new2), axis=0)
    maxrow[0] = jnp.broadcast_to(jnp.max(tops, axis=1, keepdims=True), tops.shape)

    def send_rows(k):
        pltpu.make_async_remote_copy(
            src_ref=maxrow.at[0],
            dst_ref=maxrows.at[k],
            send_sem=send_sem.at[3],
            recv_sem=recv_sem.at[3],
            device_id={"mp": lax.rem(mp + k + 1, nmp)},
            device_id_type=MESH,
        ).start()

    loop(nmp - 1, send_rows)

    ratio = new1 / fix1 / (jnp.sqrt(new2 / fix2) + 1e-8)
    old_weights = weights[...]
    new_weights = old_weights - 0.001 * (ratio + 0.1 * old_weights)
    params[dp] = new_weights.astype(jnp.bfloat16)

    def send_params(k):
        pltpu.make_async_remote_copy(
            src_ref=params.at[dp],
            dst_ref=params.at[dp],
            send_sem=send_sem.at[4],
            recv_sem=recv_sem.at[4],
            device_id={"dp": lax.rem(dp + k + 1, ndp)},
            device_id_type=MESH,
        ).start()

    loop(ndp - 1, send_params)


    def send_cols(k):
        pltpu.make_async_remote_copy(
            src_ref=maxcol.at[2],
            dst_ref=maxcols.at[k],
            send_sem=send_sem.at[2],
            recv_sem=recv_sem.at[2],
            device_id={"dp": lax.rem(dp + 2 * (k + 1), ndp)},
            device_id_type=MESH,
        ).start()

    pair.wait_recv()
    maxcol[2] = jnp.maximum(maxcol[0], maxcol[1])
    loop(ndp // 2 - 1, send_cols)
    master_out[...] = new_weights
    ratio_out[...] = ratio

    wait_all(maxrows, nmp - 1, recv_sem.at[3])
    toprow = fold(jnp.maximum, maxrow[0], maxrows, nmp - 1)
    rows_out[...] = toprow
    wait_all(maxcols, ndp // 2 - 1, recv_sem.at[2])
    topcol = fold(jnp.maximum, maxcol[2], maxcols, ndp // 2 - 1)
    cols_out[...] = topcol
    scaled1_out[...] = new1 / (scale(lambda r: toprow[r : r + 1], topcol[0]) + 1e-8)
    scaled2_out[...] = new2 / (
        scale(lambda r: toprow[rows + r : rows + r + 1], topcol[1]) + 1e-8
    )

    wait_all(params, ndp - 1, recv_sem.at[4])
    params_out[...] = params[...]

    wait_all(grads, ndp - 1, send_sem.at[0])
    wait_all(squares, ndev - 1, send_sem.at[1])
    pair.wait_send()
    wait_all(maxcols, ndp // 2 - 1, send_sem.at[2])
    wait_all(maxrows, nmp - 1, send_sem.at[3])
    wait_all(params, ndp - 1, send_sem.at[4])


def unpack(
    master,
    ratio,
    params,
    scaled1,
    scaled2,
    toprows,
    topcols,
    master_out,
    ratio_out,
    params_out,
    scaled1_out,
    scaled2_out,
    rows1_out,
    cols1_out,
    rows2_out,
    cols2_out,
    wide,
):
    rows, ncols = master_out.shape
    ndp = params.shape[0]
    parts = ncols // (SUB * LANES)
    deep = rows * SUB

    cols1_out[...] = topcols[0]
    cols2_out[...] = topcols[1]
    for r in range(rows):
        rows1_out[r] = jnp.max(toprows[r : r + 1, :])
        rows2_out[r] = jnp.max(toprows[rows + r : rows + r + 1, :])
    for j in range(ndp):
        block = params[j].astype(F32)
        for p in range(parts):
            wide[p, j * deep : (j + 1) * deep] = block[p * deep : (p + 1) * deep]
    for b in range(ncols // LANES):
        p, sub = b // SUB, b % SUB
        cols = slice(b * LANES, (b + 1) * LANES)
        part = pl.ds(p * deep + sub, rows, stride=SUB)
        master_out[:, cols] = master[part, :]
        ratio_out[:, cols] = ratio[part, :]
        scaled1_out[:, cols] = scaled1[part, :]
        scaled2_out[:, cols] = scaled2[part, :]
        params_out[:, cols] = wide[p, pl.ds(sub, ndp * rows, stride=SUB), :].astype(
            jnp.bfloat16
        )


def shards(
    ndp,
    nmp,
    hidden_input,
    output_cotangent,
    master_weights,
    first_codes,
    second_codes,
    first_rows,
    first_cols,
    second_rows,
    second_cols,
    step_count,
):
    rows, ncols = master_weights.shape
    tokens, width = hidden_input.shape
    parts = ncols // (SUB * LANES)
    loads = 2
    height = parts * rows * SUB
    hbm = pl.BlockSpec(memory_space=pltpu.HBM)
    smem = pl.BlockSpec(memory_space=pltpu.SMEM)
    vmem = pl.BlockSpec(memory_space=pltpu.VMEM)
    whole = jax.ShapeDtypeStruct((rows, ncols), F32)
    block = (height, LANES)
    line = (parts * SUB, LANES)
    dense = pltpu.VMEM(block, F32)
    results = pl.pallas_call(
        functools.partial(kernel, ndp, nmp, loads),
        out_shape=(
            dense,
            dense,
            pltpu.VMEM((ndp, *block), jnp.bfloat16),
            dense,
            dense,
            pltpu.VMEM((2 * rows, LANES), F32),
            pltpu.VMEM((2, *line), F32),
        ),
        in_specs=[hbm] * 10,
        out_specs=[vmem] * 7,
        scratch_shapes=[
            pltpu.VMEM((width, tokens), jnp.bfloat16),
            pltpu.VMEM((parts * loads, tokens, ncols // (parts * loads)), jnp.bfloat16),
            pltpu.VMEM((rows, ncols), F32),
            pltpu.VMEM((rows, ncols), jnp.int32),
            pltpu.VMEM((rows, ncols), jnp.int32),
            pltpu.VMEM(line, F32),
            pltpu.VMEM(line, F32),
            pltpu.VMEM((1, rows), F32),
            pltpu.VMEM((1, rows), F32),
            pltpu.VMEM((1, 1), jnp.int32),
            pltpu.VMEM((parts, ndp * rows * SUB, LANES), F32),
            pltpu.VMEM((ndp - 1, *block), F32),
            pltpu.VMEM((1, 1, LANES), F32),
            pltpu.VMEM((ndp * nmp - 1, 1, LANES), F32),
            pltpu.VMEM((ndp, *block), jnp.bfloat16),
            pltpu.VMEM((3, 2, *line), F32),
            pltpu.VMEM((ndp // 2 - 1, 2, *line), F32),
            pltpu.VMEM((1, 2 * rows, LANES), F32),
            pltpu.VMEM((nmp - 1, 2 * rows, LANES), F32),
            pltpu.VMEM(block, F32),
            pltpu.VMEM(block, F32),
            pltpu.VMEM(block, F32),
            pltpu.SemaphoreType.DMA((9,)),
            pltpu.SemaphoreType.DMA((parts * loads,)),
            pltpu.SemaphoreType.DMA((6,)),
            pltpu.SemaphoreType.DMA((6,)),
        ],
        compiler_params=pltpu.CompilerParams(
            collective_id=0, has_side_effects=True, vmem_limit_bytes=60 * 1024 * 1024
        ),
    )(
        hidden_input.T,
        output_cotangent,
        master_weights,
        first_codes,
        second_codes,
        first_cols.reshape(line),
        second_cols.reshape(line),
        first_rows.reshape(1, rows),
        second_rows.reshape(1, rows),
        step_count.reshape(1, 1),
    )
    scales = jax.ShapeDtypeStruct((rows,), F32)
    cols = jax.ShapeDtypeStruct(line, F32)
    outs = pl.pallas_call(
        unpack,
        out_shape=(
            whole,
            whole,
            jax.ShapeDtypeStruct((ndp * rows, ncols), jnp.bfloat16),
            whole,
            whole,
            scales,
            cols,
            scales,
            cols,
        ),
        in_specs=[vmem] * 7,
        out_specs=[vmem] * 5 + [smem, vmem] * 2,
        scratch_shapes=[pltpu.VMEM((parts, ndp * rows * SUB, LANES), F32)],
        compiler_params=pltpu.CompilerParams(vmem_limit_bytes=40 * 1024 * 1024),
    )(*results)
    return (*outs[:6], outs[6].reshape(ncols), outs[7], outs[8].reshape(ncols))


def solution(mesh):
    return jax.shard_map(
        functools.partial(shards, mesh.shape["dp"], mesh.shape["mp"]),
        mesh=mesh,
        in_specs=(
            P("dp", None),
            P("dp", "mp"),
            P("dp", "mp"),
            P("dp", "mp"),
            P("dp", "mp"),
            P("dp"),
            P("mp"),
            P("dp"),
            P("mp"),
            P(),
        ),
        out_specs=(
            P("dp", "mp"),
            P("dp", "mp"),
            P(None, "mp"),
            P("dp", "mp"),
            P("dp", "mp"),
            P("dp"),
            P("mp"),
            P("dp"),
            P("mp"),
        ),
        check_vma=False,
    )
```
